8 devices in a mesh: data: 1 (over z), inner: 2 (over y), stage: 4 (over x, core).
Axes of the slice: x: 2, y: 2, z: 1, core: 2. Of those that a mesh axis runs over, the one named last changes fastest.
Arguments:
- x: bfloat16 [8, 1024, 2048], P(('data', 'stage'), 'inner')
- g: bfloat16 [8, 1024, 2048], P(('data', 'stage'), 'inner')
- w1: bfloat16 [1, 4, 2048, 8192], P(None, 'stage')
- w2: bfloat16 [1, 4, 8192, 2048], P(None, 'stage')
Outputs:
- output 1: bfloat16 [8, 1024, 2048], P(('data', 'stage'), 'inner')
- output 2: bfloat16 [8, 1024, 2048], P(('data', 'stage'), 'inner')
- output 3: float32 [1, 4, 2048, 8192], P('data', 'stage')
- output 4: float32 [1, 4, 8192, 2048], P('data', 'stage')
All inputs are finite; a program needn't handle non-finite values.
Results may differ from the reference program's by a relative error of at most 0.0140198.
Values are sent between devices in bfloat16 or wider.
A program may use at most 1 GiB of HBM per device.

```python
import jax
import jax.numpy as jnp
from jax import lax

D = 2048
FF = 8192
V = 1
K = 1
STAGE = 4
MICRO = 8
B = 1024

LAYERS = V * STAGE * K


def setup_inputs(seed: int = 0, part: int = 0) -> dict:
    key = jax.random.PRNGKey(seed)
    kbase, kshared = jax.random.split(key)
    kx, kg = jax.random.split(jax.random.fold_in(kbase, part))
    k1, k2 = jax.random.split(kshared)
    x = jax.random.normal(kx, (MICRO, B, D), jnp.float32).astype(jnp.bfloat16)
    g = jax.random.normal(kg, (MICRO, B, D), jnp.float32).astype(jnp.bfloat16)
    w1 = (jax.random.normal(k1, (V, STAGE * K, D, FF), jnp.float32) * D ** -0.5).astype(jnp.bfloat16)
    w2 = (jax.random.normal(k2, (V, STAGE * K, FF, D), jnp.float32) * (2.0 * (FF * LAYERS) ** -0.5)).astype(jnp.bfloat16)
    return {"x": x, "g": g, "w1": w1, "w2": w2}


def _gelu(t):
    return jax.nn.gelu(t, approximate=True)


def _layer_fwd(h, w1, w2):
    z = jnp.dot(h, w1, preferred_element_type=jnp.float32)
    a = _gelu(z).astype(jnp.bfloat16)
    u = jnp.dot(a, w2, preferred_element_type=jnp.float32)
    return (h.astype(jnp.float32) + u).astype(jnp.bfloat16)


def _layer_bwd(h, dh, w1, w2):
    z = jnp.dot(h, w1, preferred_element_type=jnp.float32)
    a32, gelu_vjp = jax.vjp(_gelu, z)
    a = a32.astype(jnp.bfloat16)
    dw2 = jnp.dot(a.T, dh, preferred_element_type=jnp.float32)
    da = jnp.dot(dh, w2.T, preferred_element_type=jnp.float32)
    dz = gelu_vjp(da)[0].astype(jnp.bfloat16)
    dw1 = jnp.dot(h.T, dz, preferred_element_type=jnp.float32)
    dh_prev = (dh.astype(jnp.float32) + jnp.dot(dz, w1.T, preferred_element_type=jnp.float32)).astype(jnp.bfloat16)
    return dh_prev, dw1, dw2


def reference(x, g, w1, w2):
    w1s = w1.reshape(LAYERS, D, FF)
    w2s = w2.reshape(LAYERS, FF, D)

    def one_micro(acc, xg):
        dw1_acc, dw2_acc = acc
        xm, gm = xg

        def fwd(h, w):
            return _layer_fwd(h, w[0], w[1]), h

        y, hs = lax.scan(fwd, xm, (w1s, w2s))

        def bwd(dh, inp):
            h, a, b = inp
            dh_prev, d1, d2 = _layer_bwd(h, dh, a, b)
            return dh_prev, (d1, d2)

        dx, (d1s, d2s) = lax.scan(bwd, gm, (hs, w1s, w2s), reverse=True)
        return (dw1_acc + d1s, dw2_acc + d2s), (y, dx)

    init = (jnp.zeros((LAYERS, D, FF), jnp.float32), jnp.zeros((LAYERS, FF, D), jnp.float32))
    (dw1, dw2), (y, dx) = lax.scan(one_micro, init, (x, g))
    return y, dx, dw1.reshape(w1.shape), dw2.reshape(w2.shape)
```

```python
import jax
import jax.numpy as jnp
from jax import lax
from jax.experimental import pallas as pl
from jax.experimental.pallas import tpu as pltpu
from jax.sharding import PartitionSpec as P

F32 = jnp.float32
BF = jnp.bfloat16
NN = (((1,), (0,)), ((), ()))
NT = (((1,), (1,)), ((), ()))
TN = (((0,), (0,)), ((), ()))
C0 = 0.7978845608028654
C1 = 0.044715
VMEM_LIMIT = 60 * 2**20
LAG = 2


def _dot(a, b, dims):
    return lax.dot_general(a, b, dims, preferred_element_type=F32)


def _gelu(z):
    return z * (0.5 * (1.0 + jnp.tanh(C0 * (z + C1 * (z * z * z)))))


def _gelu_and_grad(z):
    z2 = z * z
    t = jnp.tanh(C0 * (z + C1 * (z2 * z)))
    cdf = 0.5 * (1.0 + t)
    return z * cdf, cdf + 0.5 * z * (1.0 - t * t) * (C0 * (1.0 + 3.0 * C1 * z2))


def _load(ref, slot, buf, sem):
    return pltpu.make_async_copy(ref.at[slot], buf, sem)


def _tick_call(body, stacks, args, out_shapes, scratch, flops, nbytes, name):
    n_plain = len(args)
    n_alias = 0 if stacks[0] is None else len(stacks)
    args = tuple(args) + tuple(stacks[:n_alias])
    n = len(args)
    if n_alias == 0:
        inner = body
        body = lambda *refs: inner(*refs[:n_plain], *[None] * len(stacks), *refs[n_plain:])
    hbm = pl.BlockSpec(memory_space=pl.ANY)
    return pl.pallas_call(
        body,
        in_specs=[pl.BlockSpec(memory_space=pltpu.SMEM)] + [hbm] * (n - 1),
        out_specs=[hbm] * len(out_shapes),
        out_shape=out_shapes,
        input_output_aliases={n_plain + i: i for i in range(n_alias)},
        scratch_shapes=scratch,
        compiler_params=pltpu.CompilerParams(vmem_limit_bytes=VMEM_LIMIT),
        cost_estimate=pl.CostEstimate(flops=flops, bytes_accessed=nbytes, transcendentals=0),
        name=name,
    )(*args)


def _fwd_tick(sc, k, xin, slot, inc, w1, w2, z_all, a_all, h_all, m, ft):
    d, f = w1.shape
    t = xin.shape[1]
    n = f // ft
    last = n - 1

    def body(sc_ref, x_ref, inc_ref, w1_ref, w2_ref, _z, _a, _h, z_ref, a_ref, hs_ref, ho_ref, h_v, o_v, acc, asc, sem, sem2):
        mi = sc_ref[k, 1]

        @pl.when(sc_ref[k, 0] == 1)
        def _():
            @pl.when(sc_ref[k, 2] == 1)
            def _():
                _load(x_ref, slot, h_v, sem).start()

            @pl.when(sc_ref[k, 2] == 0)
            def _():
                _load(inc_ref, 0, h_v, sem).start()

            keep = pltpu.make_async_copy(h_v, hs_ref.at[mi], sem2)

            def step(w1_b, w2_b, z_b, a_b):
                i = pl.program_id(0)

                def first_half(slot):
                    z = _dot(h_v[...], w1_b[...], NN)
                    z_b[...] = z
                    a = _gelu(z).astype(BF)
                    a_b[...] = a
                    asc[slot] = a

                @pl.when(i == 0)
                def _():
                    _load(inc_ref, 0, h_v, sem).wait()
                    keep.start()
                    first_half(0)
                    acc[...] = jnp.zeros_like(acc)

                for par in (0, 1):
                    @pl.when((i > 0) & (i < n) & (i % 2 == par))
                    def _():
                        u = _dot(asc[1 - par], w2_b[...], NN)
                        first_half(par)
                        acc[...] += u

                @pl.when(i == n)
                def _():
                    u = _dot(asc[last % 2], w2_b[...], NN)
                    o_v[...] = (h_v[...].astype(F32) + (acc[...] + u)).astype(BF)

            pltpu.emit_pipeline(
                step,
                grid=(n + 1,),
                in_specs=[
                    pl.BlockSpec((d, ft), lambda i: (0, jnp.minimum(i, last))),
                    pl.BlockSpec((ft, d), lambda i: (jnp.maximum(i - 1, 0), 0)),
                ],
                out_specs=[
                    pl.BlockSpec((t, ft), lambda i: (0, jnp.minimum(i, last))),
                    pl.BlockSpec((t, ft), lambda i: (0, jnp.minimum(i, last))),
                ],
            )(w1_ref, w2_ref, z_ref.at[mi], a_ref.at[mi])
            out = pltpu.make_async_copy(o_v, ho_ref.at[0], sem)
            out.start()
            out.wait()
            keep.wait()

    return _tick_call(
        body, [z_all, a_all, h_all], (sc, xin, inc, w1, w2),
        [jax.ShapeDtypeStruct((m, t, f), F32), jax.ShapeDtypeStruct((m, t, f), BF),
         jax.ShapeDtypeStruct((m, t, d), BF), jax.ShapeDtypeStruct((1, t, d), BF)],
        [pltpu.VMEM((t, d), BF), pltpu.VMEM((t, d), BF), pltpu.VMEM((t, d), F32), pltpu.VMEM((2, t, ft), BF),
         pltpu.SemaphoreType.DMA, pltpu.SemaphoreType.DMA],
        4 * t * d * f, 4 * d * f + 6 * t * f, "fwd_tick")


def _bwd_tick(sc, k, gin, slot, inc, w1, w2, z_all, dz_all, g_all, m, ft):
    d, f = w1.shape
    t = gin.shape[1]
    n = f // ft
    last = n - 1

    def body(sc_ref, x_ref, inc_ref, w1_ref, w2_ref, z_ref, _dz, _g, dz_ref, gs_ref, go_ref, g_v, o_v, acc, asc, sem, sem2):
        mi = sc_ref[k, 1]

        @pl.when(sc_ref[k, 0] == 1)
        def _():
            @pl.when(sc_ref[k, 2] == 1)
            def _():
                _load(x_ref, slot, g_v, sem).start()

            @pl.when(sc_ref[k, 2] == 0)
            def _():
                _load(inc_ref, 0, g_v, sem).start()

            keep = pltpu.make_async_copy(g_v, gs_ref.at[mi], sem2)

            def step(w1_b, w2_b, z_b, dz_b):
                i = pl.program_id(0)

                def first_half(slot):
                    da = _dot(g_v[...], w2_b[...], NT)
                    _, slope = _gelu_and_grad(z_b[...])
                    dz = (da * slope).astype(BF)
                    dz_b[...] = dz
                    asc[slot] = dz

                @pl.when(i == 0)
                def _():
                    _load(inc_ref, 0, g_v, sem).wait()
                    keep.start()
                    first_half(0)
                    acc[...] = jnp.zeros_like(acc)

                for par in (0, 1):
                    @pl.when((i > 0) & (i < n) & (i % 2 == par))
                    def _():
                        u = _dot(asc[1 - par], w1_b[...], NT)
                        first_half(par)
                        acc[...] += u

                @pl.when(i == n)
                def _():
                    u = _dot(asc[last % 2], w1_b[...], NT)
                    o_v[...] = (g_v[...].astype(F32) + (acc[...] + u)).astype(BF)

            pltpu.emit_pipeline(
                step,
                grid=(n + 1,),
                in_specs=[
                    pl.BlockSpec((d, ft), lambda i: (0, jnp.maximum(i - 1, 0))),
                    pl.BlockSpec((ft, d), lambda i: (jnp.minimum(i, last), 0)),
                    pl.BlockSpec((t, ft), lambda i: (0, jnp.minimum(i, last))),
                ],
                out_specs=[pl.BlockSpec((t, ft), lambda i: (0, jnp.minimum(i, last)))],
            )(w1_ref, w2_ref, z_ref.at[mi], dz_ref.at[mi])
            out = pltpu.make_async_copy(o_v, go_ref.at[0], sem)
            out.start()
            out.wait()
            keep.wait()

    return _tick_call(
        body, [dz_all, g_all], (sc, gin, inc, w1, w2, z_all),
        [jax.ShapeDtypeStruct((m, t, f), BF), jax.ShapeDtypeStruct((m, t, d), BF),
         jax.ShapeDtypeStruct((1, t, d), BF)],
        [pltpu.VMEM((t, d), BF), pltpu.VMEM((t, d), BF), pltpu.VMEM((t, d), F32), pltpu.VMEM((2, t, ft), BF),
         pltpu.SemaphoreType.DMA, pltpu.SemaphoreType.DMA],
        4 * t * d * f, 4 * d * f + 6 * t * f, "bwd_tick")


def _peer_grads(h, g, base, w1, w2, dw1, dw2, ft, tc):
    t, d = g.shape
    f = w1.shape[1]
    nc = t // tc

    def body(h_ref, g_ref, w1_ref, w2_ref, d1_in, d2_in, d1_ref, d2_ref):
        z = _dot(h_ref[...], w1_ref[...], NN)
        da = _dot(g_ref[...], w2_ref[...], NT)
        a, slope = _gelu_and_grad(z)
        u1 = _dot(h_ref[...], (da * slope).astype(BF), TN)
        u2 = _dot(a.astype(BF), g_ref[...], TN)

        @pl.when(pl.program_id(1) == 0)
        def _():
            d1_ref[...] = d1_in[...] + u1
            d2_ref[...] = d2_in[...] + u2

        @pl.when(pl.program_id(1) > 0)
        def _():
            d1_ref[...] += u1
            d2_ref[...] += u2

    tok = pl.BlockSpec((tc, d), lambda i, c: (c, 0))
    col = pl.BlockSpec((d, ft), lambda i, c: (0, i))
    row = pl.BlockSpec((ft, d), lambda i, c: (i, 0))
    return pl.pallas_call(
        body, grid=(f // ft, nc),
        in_specs=[pl.BlockSpec((tc, d), lambda i, c: (c + base // tc, 0)), tok, col, row, col, row],
        out_specs=[col, row],
        out_shape=[jax.ShapeDtypeStruct((d, f), F32), jax.ShapeDtypeStruct((f, d), F32)],
        input_output_aliases={4: 0, 5: 1},
        compiler_params=pltpu.CompilerParams(vmem_limit_bytes=VMEM_LIMIT),
        cost_estimate=pl.CostEstimate(flops=8 * t * d * f, bytes_accessed=20 * d * f, transcendentals=0),
        name="peer_grads",
    )(h, g, w1, w2, dw1, dw2)


def solution(mesh):
    n_stage = mesh.shape["stage"]
    n_inner = mesh.shape["inner"]
    assert n_stage == 4 and n_inner == 2
    up = [(i, i + 1) for i in range(n_stage - 1)]
    down = [(i, i - 1) for i in range(n_stage - 1, 0, -1)]
    swap = [(0, 1), (1, 0)]

    def body(x, g, w1, w2):
        p = lax.axis_index("stage")
        mb, t, d = x.shape
        w1, w2 = w1[0, 0], w2[0, 0]
        f = w1.shape[1]
        m = mb * n_stage
        last = n_stage - 1
        ft = min(1024, f // 2)
        ticks = m + LAG * last

        def table(first_stage, reverse):
            item = jnp.arange(ticks, dtype=jnp.int32) - LAG * first_stage
            ok = (item >= 0) & (item < m)
            at = jnp.clip(item, 0, m - 1)
            at = m - 1 - at if reverse else at
            first = jnp.broadcast_to(first_stage == 0, item.shape)
            return jnp.stack([ok.astype(jnp.int32), at, first.astype(jnp.int32)], axis=1)

        def hop(val, k, hops):
            return lax.ppermute(val, "stage", [hops[s] for s in range(last) if 0 <= k - LAG * s < m])

        def after(val, event):
            return lax.optimization_barrier((val, event))[0]

        xs = [x] + [lax.ppermute(x, "stage", [(s, 0)]) for s in range(1, n_stage)]
        z_all = a_all = h_all = None
        incs = {}
        outs = {}
        gs = {last: g}
        gs_at = {k: s for k, s in zip((LAG + 2, LAG + 3, LAG + 5), reversed(range(last)))}
        sc = table(p, False)
        for k in range(ticks):
            item = min(k, m - 1)
            z_all, a_all, h_all, ho = _fwd_tick(
                sc, k, xs[item // mb], item % mb, incs.pop(k - LAG, x), w1, w2, z_all, a_all, h_all, m, ft)
            if k < ticks - LAG:
                incs[k] = hop(ho, k, up)
            if k in gs_at:
                gs[gs_at[k]] = lax.ppermute(after(g, ho), "stage", [(gs_at[k], last)])
            outs[k - LAG * last] = ho
        y_own = {j: outs[j] for j in range(m)}
        y_far = {j: lax.ppermute(after(y_own[j], h_all), "stage", [(last, j // mb)]) for j in range(m - mb)}
        h_peer = lax.ppermute(h_all, "inner", swap)

        dz_all = g_all = None
        half = m // 2
        g_peer = {}
        incs = {}
        outs = {}
        sc = table(last - p, True)
        for k in range(ticks):
            item = m - 1 - min(k, m - 1)
            dz_all, g_all, go = _bwd_tick(
                sc, k, gs[item // mb], item % mb, incs.pop(k - LAG, x), w1, w2, z_all, dz_all, g_all, m, ft)
            if k < ticks - LAG:
                incs[k] = hop(go, k, down)
            outs[m - 1 - (k - LAG * last)] = go
            if k == LAG * last + half - 1:
                g_peer[1] = lax.ppermute(g_all[half:], "inner", swap)
        g_peer[0] = lax.ppermute(g_all[:half], "inner", swap)
        dx_own = {j: outs[j] for j in range(m)}
        dx_far = {j: lax.ppermute(after(dx_own[j], g_all), "stage", [(0, j // mb)]) for j in range(mb, m)}

        def gather_out(own, far, home):
            rows = []
            for s in range(mb):
                r = own[home * mb + s]
                for st in range(n_stage):
                    if st != home:
                        r = jnp.where(p == st, far[st * mb + s], r)
                rows.append(r)
            return jnp.concatenate(rows, axis=0)

        y = gather_out(y_own, y_far, last)
        dx = gather_out(dx_own, dx_far, 0)

        flat = lambda v: v.reshape(-1, v.shape[-1])
        dw1 = _dot(flat(h_all), flat(dz_all), TN)
        dw2 = _dot(flat(a_all), flat(g_all), TN)
        for i in (1, 0):
            dw1, dw2 = _peer_grads(
                flat(h_peer), flat(g_peer[i]), i * half * t, w1, w2, dw1, dw2, min(256, f), min(1024, half * t))
        return y, dx, dw1[None, None], dw2[None, None]

    tok = P(("data", "stage"), "inner", None)
    wsp = P(None, "stage", None, None)
    dsp = P("data", "stage", None, None)
    return jax.shard_map(body, mesh=mesh, in_specs=(tok, tok, wsp, wsp), out_specs=(tok, tok, dsp, dsp), check_vma=False)
```
